32 devices in a mesh: ctx: 8 (over y, x, core), tp: 4 (over z).
Axes of the slice: x: 2, y: 2, z: 4, core: 2. Of those that a mesh axis runs over, the one named last changes fastest.
Arguments:
- tokens: bfloat16 [4096, 4096], P('ctx'), may hold values from -48 to 48
- w_query: bfloat16 [4096, 4096], P(None, 'tp'), may hold values from -0.09375 to 0.09375
- w_key: bfloat16 [4096, 4096], P(None, 'tp'), may hold values from -0.09375 to 0.09375
- w_value: bfloat16 [4096, 4096], P(None, 'tp'), may hold values from -0.09375 to 0.09375
- w_out: bfloat16 [4096, 4096], P('tp'), may hold values from -0.09375 to 0.09375
- block_doc: int32 [64], replicated, may hold values from 0 to 1, never falling along the last dimension, each value on 1 to 56 neighbouring positions
- grad_out: bfloat16 [4096, 4096], P('ctx', 'tp'), may hold values from -6 to 6
Outputs:
- output: bfloat16 [4096, 4096], P('ctx', 'tp')
- grad_tokens: bfloat16 [4096, 4096], P('ctx', 'tp')
- grad_query_weight: float32 [4096, 4096], P('ctx', 'tp')
- grad_key_weight: float32 [4096, 4096], P('ctx', 'tp')
- grad_value_weight: float32 [4096, 4096], P('ctx', 'tp')
- grad_out_weight: float32 [4096, 4096], P('tp', 'ctx')
The draws below stay inside these ranges and needn't reach their ends.
Inputs may be any that keep to these rules, and one draw needn't show every extreme that they name: block_doc never falls along the blocks; each document covers 1 to 56 consecutive blocks.
All inputs are finite; a program needn't handle non-finite values.
Results may differ from the reference program's by a relative error of at most 0.024.
The reference program's roundings to bfloat16 on the way count: a program that leaves them out, or rounds other values in their place, can miss the bound.
Values may be sent and summed in bfloat16 or wider, within the bound.
No kernel may reach another device: no remote copies, remote signals or barrier semaphores. Data moves between devices by JAX's collectives and lax.ppermute only.
A program may use at most 192 MiB of HBM per device.

```python
import math
import jax
import jax.numpy as jnp
import numpy as np
from jax import lax

D = 4096
HEADS = 32
HDIM = 128
BLOCK = 64
SEQ = 4096
NBLK = 64
N_CTX = 8


def draw_tokens(key, part):
    normal_part = jnp.clip(jax.random.normal(key, (SEQ, D), jnp.float32), -6.0, 6.0)
    return normal_part.astype(jnp.bfloat16)


def level_of(own_key, shape, shards, least, top_value):
    def one(axis_at, shards_of):
        draws = jax.random.uniform(jax.random.fold_in(jax.random.fold_in(own_key, 6), axis_at), (shards_of,), jnp.float32, least / len(shards), top_value / len(shards))
        return jnp.repeat(jnp.exp(draws), shape[axis_at] // shards_of).reshape((-1,) + (1,) * (len(shape) - axis_at - 1))

    gain = one(*shards[0])
    for cut in shards[1:]:
        gain = gain * one(*cut)
    return gain


def profile(number_of, total, reach, lean):
    loads = [(1 << 20) // math.isqrt(standing ** lean) + 1 for standing in range(2, number_of + 1)]
    spare, given = total - reach - (number_of - 1), [1] * (number_of - 1)
    while spare > 0:
        candidates = [i for i in range(number_of - 1) if given[i] < reach]
        mass, budget = sum([loads[i] for i in candidates]), spare
        for i in candidates:
            extra = min(reach - given[i], max(1, budget * loads[i] // mass), spare)
            given[i] = given[i] + extra
            spare = spare - extra
    return np.array([reach] + given)


def ragged(own_key, number_of, total, reach, slope):
    if number_of == 2:
        one = jax.random.randint(own_key, (), max(1, total - reach), min(reach, total - 1) + 1)
        return jnp.stack([one, total - one])
    lengths = jnp.asarray(profile(number_of, total, reach, slope), jnp.int32)
    pairs = (number_of - 1) // 2
    giver, receiver = lengths[1:1 + 2 * pairs:2], lengths[2:2 + 2 * pairs:2]
    margin = jnp.minimum(giver - 1, reach - receiver)
    moved = jax.random.randint(jax.random.fold_in(own_key, 1), (pairs,), 0, 1 << 20) % (margin + 1)
    lengths = lengths.at[1:1 + 2 * pairs:2].set(giver - moved).at[2:2 + 2 * pairs:2].set(receiver + moved)
    return lengths[jax.random.permutation(jax.random.fold_in(own_key, 2), number_of)]


def bell_draw(key, shape, spread, limit, split=(), kind=jnp.bfloat16):
    loudness = level_of(key, shape, split, -0.22, 0.18) if split else 1.0
    entries = jax.random.normal(key, shape, jnp.float32) * spread * loudness
    return jnp.minimum(jnp.maximum(entries, -limit), limit).astype(kind)


def setup_inputs(seed: int = 0) -> dict:
    seeds = jax.random.split(jax.random.key(seed), 8)
    tokens = draw_tokens(jax.random.fold_in(seeds[7], 71), 0)
    w_query = bell_draw(seeds[1], (D, D), D ** -0.5, 0.09375, ((1, 4),))
    w_key = bell_draw(seeds[2], (D, D), D ** -0.5, 0.09375, ((1, 4),))
    w_value = bell_draw(seeds[3], (D, D), D ** -0.5, 0.09375, ((1, 4),))
    w_out = bell_draw(seeds[4], (D, D), D ** -0.5, 0.09375, ((0, 4),))
    block_doc = jnp.searchsorted(jnp.cumsum(ragged(seeds[5], 2, NBLK, NBLK - NBLK // 8, 1)), jnp.arange(NBLK), side="right").astype(jnp.int32)
    grad_out = bell_draw(seeds[6], (SEQ, D), 1.0, 6.0, ((0, 8), (1, 4)))
    return {"tokens": tokens, "w_query": w_query, "w_key": w_key, "w_value": w_value, "w_out": w_out, "block_doc": block_doc, "grad_out": grad_out}


big_negative = -1e+30

def elementwise_product(pattern, left_side, right_side):
    left_side, right_side = lax.optimization_barrier((left_side, right_side))
    return jnp.einsum(pattern, left_side.astype(jnp.float32), right_side.astype(jnp.float32), precision=lax.Precision.HIGHEST)

def attend(query_row_matrix, key_row_matrix, value_row_matrix, summary_key, summary_value, allowed, causal, score_scale_factor):
    near_scores = elementwise_product('nqhd,nkhd->nhqk', query_row_matrix, key_row_matrix) * score_scale_factor
    near_scores = jnp.where(causal[None, None], near_scores, big_negative)
    distant_score_matrix = elementwise_product('yzxo,lxo->yzxl', query_row_matrix, summary_key) * score_scale_factor
    distant_score_matrix = jnp.where(allowed[:, None, None, :], distant_score_matrix, big_negative)
    row_top = jnp.maximum(jnp.transpose(lax.optimization_barrier(jnp.max(near_scores, axis=3)), (0, 2, 1)), lax.optimization_barrier(jnp.max(distant_score_matrix, axis=3)))
    near_exp = jnp.exp(near_scores - jnp.transpose(row_top, (0, 2, 1))[..., None])
    far_exp = jnp.exp(distant_score_matrix - row_top[..., None])
    denom_sum = jnp.transpose(lax.optimization_barrier(jnp.sum(near_exp, axis=3)), (0, 2, 1)) + lax.optimization_barrier(jnp.sum(far_exp, axis=3))
    local_weight = (near_exp / jnp.transpose(denom_sum, (0, 2, 1))[..., None]).astype(jnp.bfloat16)
    distant_weight = (far_exp / denom_sum[..., None]).astype(jnp.bfloat16)
    combined_output = elementwise_product('jvyb,jbvo->jyvo', local_weight, value_row_matrix) + elementwise_product('gtuv,vuk->gtuk', distant_weight, summary_value)
    return (combined_output.astype(jnp.bfloat16), local_weight, distant_weight)

def attend_back(query_row_matrix, key_row_matrix, value_row_matrix, summary_key, summary_value, combined_output, local_weight, distant_weight, incoming_gradient, score_scale_factor):
    pair = lax.optimization_barrier((combined_output, incoming_gradient))
    row_delta = lax.optimization_barrier(jnp.sum(pair[0].astype(jnp.float32) * pair[1].astype(jnp.float32), axis=3))
    near_d = elementwise_product('nqhd,nkhd->nhqk', incoming_gradient, value_row_matrix)
    distant_gradient_term = elementwise_product('yzxo,lxo->yzxl', incoming_gradient, summary_value)
    weights = lax.optimization_barrier((local_weight, distant_weight))
    local_score_sum = (weights[0].astype(jnp.float32) * (near_d - jnp.transpose(row_delta, (0, 2, 1))[..., None])).astype(jnp.bfloat16)
    distant_score_sum = (weights[1].astype(jnp.float32) * (distant_gradient_term - row_delta[..., None])).astype(jnp.bfloat16)
    query_gradient = (elementwise_product('jvyb,jbvo->jyvo', local_score_sum, key_row_matrix) + elementwise_product('gtuv,vuk->gtuk', distant_score_sum, summary_key)) * score_scale_factor
    d_key = elementwise_product('nhqk,nqhd->nkhd', local_score_sum, query_row_matrix) * score_scale_factor
    d_value = elementwise_product('nhqk,nqhd->nkhd', local_weight, incoming_gradient)
    summary_key_gradient = elementwise_product('agwi,agwu->iwu', distant_score_sum, query_row_matrix) * score_scale_factor
    summary_value_gradient = elementwise_product('agwi,agwu->iwu', distant_weight, incoming_gradient)
    return (query_gradient, d_key, d_value, summary_key_gradient, summary_value_gradient)

def shard_sum(left_side, right_side):
    shard_rows = left_side.shape[0] // N_CTX

    def add_shard(shard_index, running):
        begin = (shard_index * shard_rows).astype(jnp.int32)
        left_part = lax.dynamic_slice_in_dim(left_side, begin, shard_rows, 0)
        right_part = lax.dynamic_slice_in_dim(right_side, begin, shard_rows, 0)
        term_rows = lax.dot_general(left_part, right_part, (((0,), (0,)), ((), ())), preferred_element_type=jnp.float32)
        term_rows = lax.optimization_barrier(term_rows.astype(jnp.bfloat16))
        return running + term_rows.astype(jnp.float32)
    start_value = jnp.zeros((left_side.shape[1], right_side.shape[1]), jnp.float32)
    return lax.fori_loop(0, N_CTX, add_shard, start_value)

def back_project(grad_rows, weight):
    return lax.dot_general(grad_rows, weight, (((1,), (1,)), ((), ())), preferred_element_type=jnp.float32)

def reference(tokens, w_query, w_key, w_value, w_out, block_doc, grad_out):
    score_scale_factor = 1.0 / math.sqrt(HDIM)
    tok_rows = tokens.shape[0]
    blocks = tok_rows // BLOCK
    block_shape = (blocks, BLOCK, HEADS, HDIM)

    def project(weight):
        return jnp.dot(tokens, weight, preferred_element_type=jnp.float32).astype(jnp.bfloat16)
    query_row_matrix = project(w_query).reshape(block_shape)
    key_row_matrix = project(w_key).reshape(block_shape)
    value_row_matrix = project(w_value).reshape(block_shape)
    summary_key = key_row_matrix[:, BLOCK - 1]
    summary_value = value_row_matrix[:, BLOCK - 1]
    block_ids = jnp.arange(blocks, dtype=jnp.int32)
    allowed = (block_ids[None, :] < block_ids[:, None]) & (block_doc[None, :] == block_doc[:, None])
    positions = jnp.arange(BLOCK, dtype=jnp.int32)
    causal = positions[None, :] <= positions[:, None]
    combined_output, local_weight, distant_weight = attend(query_row_matrix, key_row_matrix, value_row_matrix, summary_key, summary_value, allowed, causal, score_scale_factor)
    attn = combined_output.reshape(tok_rows, D)
    output = (tokens.astype(jnp.float32) + jnp.dot(attn, w_out, preferred_element_type=jnp.float32)).astype(jnp.bfloat16)
    d_attn = back_project(grad_out, w_out).astype(jnp.bfloat16)
    grads = attend_back(query_row_matrix, key_row_matrix, value_row_matrix, summary_key, summary_value, combined_output, local_weight, distant_weight, d_attn.reshape(block_shape), score_scale_factor)
    query_gradient, d_key, d_value, summary_key_gradient, summary_value_gradient = grads
    query_gradient = query_gradient.astype(jnp.bfloat16).reshape(tok_rows, D)
    d_key = d_key.at[:, BLOCK - 1].add(summary_key_gradient).astype(jnp.bfloat16).reshape(tok_rows, D)
    d_value = d_value.at[:, BLOCK - 1].add(summary_value_gradient).astype(jnp.bfloat16).reshape(tok_rows, D)
    grad_tokens = grad_out.astype(jnp.float32) + back_project(query_gradient, w_query) + back_project(d_key, w_key) + back_project(d_value, w_value)
    grad_tokens = grad_tokens.astype(jnp.bfloat16)
    return (output, grad_tokens, shard_sum(tokens, query_gradient), shard_sum(tokens, d_key), shard_sum(tokens, d_value), shard_sum(attn, grad_out))
```

```python
import math

import jax
import jax.numpy as jnp
from jax import lax
from jax.sharding import PartitionSpec as P

HDIM = 128
BLOCK = 64


big_negative = -1e30


def elementwise_product(pattern, left_side, right_side):
    return jnp.einsum(pattern, left_side, right_side, preferred_element_type=jnp.float32)


def attend(
    query_row_matrix,
    key_row_matrix,
    value_row_matrix,
    summary_key,
    summary_value,
    allowed,
    causal,
    score_scale_factor,
):
    near_scores = (
        elementwise_product("nqhd,nkhd->nhqk", query_row_matrix, key_row_matrix)
        * score_scale_factor
    )
    near_scores = jnp.where(causal[None, None], near_scores, big_negative)
    distant_score_matrix = (
        elementwise_product("yzxo,lxo->yzxl", query_row_matrix, summary_key) * score_scale_factor
    )
    distant_score_matrix = jnp.where(allowed[:, None, None, :], distant_score_matrix, big_negative)
    row_top = jnp.maximum(
        jnp.transpose(jnp.max(near_scores, axis=3), (0, 2, 1)),
        jnp.max(distant_score_matrix, axis=3),
    )
    near_exp = jnp.exp(near_scores - jnp.transpose(row_top, (0, 2, 1))[..., None])
    far_exp = jnp.exp(distant_score_matrix - row_top[..., None])
    denom_sum = jnp.transpose(jnp.sum(near_exp, axis=3), (0, 2, 1)) + jnp.sum(far_exp, axis=3)
    local_weight = (near_exp / jnp.transpose(denom_sum, (0, 2, 1))[..., None]).astype(jnp.bfloat16)
    distant_weight = (far_exp / denom_sum[..., None]).astype(jnp.bfloat16)
    combined_output = elementwise_product(
        "jvyb,jbvo->jyvo", local_weight, value_row_matrix
    ) + elementwise_product("gtuv,vuk->gtuk", distant_weight, summary_value)
    return (combined_output.astype(jnp.bfloat16), local_weight, distant_weight)


def attend_back(
    query_row_matrix,
    key_row_matrix,
    value_row_matrix,
    summary_key,
    summary_value,
    combined_output,
    local_weight,
    distant_weight,
    incoming_gradient,
    score_scale_factor,
):
    row_delta = jnp.sum(
        combined_output.astype(jnp.float32) * incoming_gradient.astype(jnp.float32), axis=3
    )
    near_d = elementwise_product("nqhd,nkhd->nhqk", incoming_gradient, value_row_matrix)
    distant_gradient_term = elementwise_product("yzxo,lxo->yzxl", incoming_gradient, summary_value)
    local_score_sum = (
        local_weight.astype(jnp.float32) * (near_d - jnp.transpose(row_delta, (0, 2, 1))[..., None])
    ).astype(jnp.bfloat16)
    distant_score_sum = (
        distant_weight.astype(jnp.float32) * (distant_gradient_term - row_delta[..., None])
    ).astype(jnp.bfloat16)
    query_gradient = (
        elementwise_product("jvyb,jbvo->jyvo", local_score_sum, key_row_matrix)
        + elementwise_product("gtuv,vuk->gtuk", distant_score_sum, summary_key)
    ) * score_scale_factor
    d_key = (
        elementwise_product("nhqk,nqhd->nkhd", local_score_sum, query_row_matrix)
        * score_scale_factor
    )
    d_value = elementwise_product("nhqk,nqhd->nkhd", local_weight, incoming_gradient)
    summary_key_gradient = (
        elementwise_product("agwi,agwu->iwu", distant_score_sum, query_row_matrix)
        * score_scale_factor
    )
    summary_value_gradient = elementwise_product(
        "agwi,agwu->iwu", distant_weight, incoming_gradient
    )
    return (query_gradient, d_key, d_value, summary_key_gradient, summary_value_gradient)


def back_project(grad_rows, weight):
    return lax.dot_general(
        grad_rows, weight, (((1,), (1,)), ((), ())), preferred_element_type=jnp.float32
    )


def term_maker(tokens, grad_rows):
    return lax.dot_general(
        tokens, grad_rows, (((0,), (0,)), ((), ())), preferred_element_type=jnp.float32
    )


def ring_scatter(partial, shard_width, axis):
    count = lax.axis_size(axis)
    me = lax.axis_index(axis)
    half = shard_width // 2
    rows = partial.shape[0]

    def piece(chunk, side):
        begin = jnp.mod(chunk, count) * shard_width + side * half
        return lax.dynamic_slice(partial, (jnp.int32(0), begin.astype(jnp.int32)), (rows, half))

    sums = []
    for side, way in ((0, 1), (1, -1)):
        pairs = [(i, (i + way) % count) for i in range(count)]
        running = piece(me - way, side)
        for step in range(count - 1):
            arrived = lax.ppermute(running.astype(jnp.bfloat16), axis, pairs)
            running = arrived.astype(jnp.float32) + piece(me - way * (step + 2), side)
        sums.append(running)
    return jnp.concatenate(sums, axis=1)


def per_device(tokens, w_query, w_key, w_value, w_out, block_doc, grad_out):
    score_scale_factor = 1.0 / math.sqrt(HDIM)
    tok_rows = tokens.shape[0]
    col_count = w_query.shape[1]
    blocks = tok_rows // BLOCK
    head_count = col_count // HDIM
    block_shape = (blocks, BLOCK, head_count, HDIM)

    def project(weight):
        return jnp.dot(tokens, weight, preferred_element_type=jnp.float32).astype(jnp.bfloat16)

    query_row_matrix = project(w_query).reshape(block_shape)
    key_row_matrix = project(w_key).reshape(block_shape)
    value_row_matrix = project(w_value).reshape(block_shape)
    own_key = key_row_matrix[:, BLOCK - 1].reshape(blocks, col_count)
    own_value = value_row_matrix[:, BLOCK - 1].reshape(blocks, col_count)
    summaries = lax.all_gather(
        jnp.concatenate([own_key, own_value], axis=1), "ctx", axis=0, tiled=True
    )
    summary_key, summary_value = summaries[:, :col_count], summaries[:, col_count:]
    total_blocks = summary_key.shape[0]
    summary_key = summary_key.reshape(total_blocks, head_count, HDIM)
    summary_value = summary_value.reshape(total_blocks, head_count, HDIM)
    first_block = lax.axis_index("ctx") * blocks
    query_ids = first_block + jnp.arange(blocks, dtype=jnp.int32)
    own_doc = lax.dynamic_slice_in_dim(block_doc, first_block, blocks, 0)
    block_ids = jnp.arange(total_blocks, dtype=jnp.int32)
    allowed = (block_ids[None, :] < query_ids[:, None]) & (block_doc[None, :] == own_doc[:, None])
    positions = jnp.arange(BLOCK, dtype=jnp.int32)
    causal = positions[None, :] <= positions[:, None]
    combined_output, local_weight, distant_weight = attend(
        query_row_matrix,
        key_row_matrix,
        value_row_matrix,
        summary_key,
        summary_value,
        allowed,
        causal,
        score_scale_factor,
    )
    attn = combined_output.reshape(tok_rows, col_count)
    partial_value = jnp.dot(attn, w_out, preferred_element_type=jnp.float32)
    shard_width = grad_out.shape[1]
    summed = ring_scatter(partial_value, shard_width, "tp")
    residual = lax.dynamic_slice_in_dim(tokens, lax.axis_index("tp") * shard_width, shard_width, 1)
    output = (residual.astype(jnp.float32) + summed).astype(jnp.bfloat16)
    upstream_full = lax.all_gather(grad_out, "tp", axis=1, tiled=True)
    out_term = lax.dot_general(
        attn, upstream_full, (((0,), (0,)), ((), ())), preferred_element_type=jnp.float32
    )
    upstream_full, out_term = lax.optimization_barrier((upstream_full, out_term.astype(jnp.bfloat16)))
    grad_out_weight = lax.psum_scatter(
        out_term, "ctx", scatter_dimension=1, tiled=True
    ).astype(jnp.float32)
    d_attn = back_project(upstream_full, w_out).astype(jnp.bfloat16)
    grads = attend_back(
        query_row_matrix,
        key_row_matrix,
        value_row_matrix,
        summary_key,
        summary_value,
        combined_output,
        local_weight,
        distant_weight,
        d_attn.reshape(block_shape),
        score_scale_factor,
    )
    query_gradient, d_key, d_value, summary_key_gradient, summary_value_gradient = grads
    flat_key = summary_key_gradient.reshape(total_blocks, col_count)
    flat_value = summary_value_gradient.reshape(total_blocks, col_count)
    ctx_count = lax.axis_size("ctx")
    flat_both = jnp.concatenate([flat_key, flat_value], axis=1)
    back_both = lax.all_to_all(
        flat_both.reshape(ctx_count, blocks, 2 * col_count), "ctx", 0, 0, tiled=True
    ).sum(axis=0)
    back_key, back_value = back_both[:, :col_count], back_both[:, col_count:]
    query_gradient = query_gradient.astype(jnp.bfloat16).reshape(tok_rows, col_count)
    d_key = (
        d_key.at[:, BLOCK - 1]
        .add(back_key.reshape(blocks, head_count, HDIM))
        .astype(jnp.bfloat16)
        .reshape(tok_rows, col_count)
    )
    d_value = (
        d_value.at[:, BLOCK - 1]
        .add(back_value.reshape(blocks, head_count, HDIM))
        .astype(jnp.bfloat16)
        .reshape(tok_rows, col_count)
    )
    d_partial = (
        back_project(query_gradient, w_query)
        + back_project(d_key, w_key)
        + back_project(d_value, w_value)
    )
    d_summed = ring_scatter(d_partial, shard_width, "tp")
    grad_tokens = (grad_out.astype(jnp.float32) + d_summed).astype(jnp.bfloat16)

    def weight_grad(grad_rows):
        term = term_maker(tokens, grad_rows).astype(jnp.bfloat16)
        return lax.psum_scatter(term, "ctx", scatter_dimension=0, tiled=True).astype(jnp.float32)

    grad_query_weight = weight_grad(query_gradient)
    grad_key_weight = weight_grad(d_key)
    grad_value_weight = weight_grad(d_value)
    return (
        output,
        grad_tokens,
        grad_query_weight,
        grad_key_weight,
        grad_value_weight,
        grad_out_weight,
    )


def solution(mesh):
    in_specs = (
        P("ctx", None),
        P(None, "tp"),
        P(None, "tp"),
        P(None, "tp"),
        P("tp", None),
        P(),
        P("ctx", "tp"),
    )
    out_specs = (
        P("ctx", "tp"),
        P("ctx", "tp"),
        P("ctx", "tp"),
        P("ctx", "tp"),
        P("ctx", "tp"),
        P("tp", "ctx"),
    )
    return jax.shard_map(
        per_device, mesh=mesh, in_specs=in_specs, out_specs=out_specs, check_vma=False
    )
```
